32 devices in a mesh: layer: 4 (over y, x), latent: 8 (over z, core).
Axes of the slice: x: 2, y: 2, z: 4, core: 2. Of those that a mesh axis runs over, the one named last changes fastest.
Arguments:
- acts: bfloat16 [128, 4, 2304], P('latent', 'layer'), may hold values from -6 to 6
- enc_weight: bfloat16 [4, 2304, 4096], P('layer', None, 'latent'), may hold values from -0.0625 to 0.0625
- enc_bias: float32 [4096], P('latent'), may hold values from -3 to 3
- dec_weight: bfloat16 [4, 4096, 2304], P('layer', 'latent'), may hold values from -0.125 to 0.125
- dec_bias: float32 [4, 2304], P('layer'), may hold values from -4 to 4
Outputs:
- recon: bfloat16 [128, 4, 2304], P('latent', 'layer')
The draws below stay inside these ranges and needn't reach their ends.
All inputs are finite; a program needn't handle non-finite values.
Results may differ from the reference program's by a relative error of at most 0.023.
Values may be sent and summed in bfloat16 or wider, within the bound.
No kernel may reach another device: no remote copies, remote signals or barrier semaphores. Data moves between devices by JAX's collectives and lax.ppermute only.
A program may use at most 64 MiB of HBM per device.

```python
import jax
import jax.numpy as jnp
from jax import lax

D = 2304
LAT_DEV = 512
LAYERS = 4
LATENTS = 4096
TOKENS = 128
N_LATENT = 8


def levels(own_key, shape, cuts, smallest, high):
    level, own = 1.0, jax.random.fold_in(own_key, 6)
    for axis_at, parts in cuts:
        steps = jnp.exp(jax.random.uniform(jax.random.fold_in(own, axis_at), (parts,), jnp.float32, smallest / len(cuts), high / len(cuts)))
        level = level * jnp.repeat(steps, shape[axis_at] // parts).reshape([-1 if axis == axis_at else 1 for axis in range(len(shape))])
    return level


def scatter_about(key, extent, spread, limit, cuts=(), held_as=jnp.bfloat16):
    array = spread * jax.random.normal(key, extent, jnp.float32)
    if cuts:
        array = array * levels(key, extent, cuts, -0.22, 0.18)
    return jnp.clip(array, -limit, limit).astype(held_as)


def setup_inputs(seed: int = 0) -> dict:
    streams_of = jax.random.split(jax.random.key(seed), 6)
    return {
        "acts": scatter_about(streams_of[0], (TOKENS, LAYERS, D), 1.0, 6.0, ((0, 8), (1, 4))),
        "enc_weight": scatter_about(streams_of[1], (LAYERS, D, LATENTS), (LAYERS * D) ** -0.5, 0.0625, ((0, 4), (2, 8))),
        "enc_bias": scatter_about(streams_of[2], (LATENTS,), 0.5, 3.0, ((0, 8),), jnp.float32),
        "dec_weight": scatter_about(streams_of[3], (LAYERS, LATENTS, D), (LATENTS // 2) ** -0.5, 0.125, ((0, 4), (1, 8))),
        "dec_bias": scatter_about(streams_of[4], (LAYERS, D), 1.0, 4.0, ((0, 4),), jnp.float32),
    }


def reference(acts, enc_weight, enc_bias, dec_weight, dec_bias):
    def encode_layer(carry, pair):
        rows, weight = pair
        return carry + jnp.dot(rows, weight, preferred_element_type=jnp.float32), None

    start = jnp.zeros((TOKENS, LATENTS), jnp.float32)
    pre, _ = lax.scan(encode_layer, start, (jnp.transpose(acts, (1, 0, 2)), enc_weight))
    codes = jnp.maximum(pre + enc_bias[None, :], 0.0).astype(jnp.bfloat16)
    code_panels = jnp.transpose(codes.reshape(TOKENS, N_LATENT, LAT_DEV), (1, 0, 2))
    dec_panels = jnp.transpose(dec_weight.reshape(LAYERS, N_LATENT, LAT_DEV, D), (1, 0, 2, 3))

    def decode_panel(carry, pair):
        panel_codes, panel_weight = pair
        term = jnp.einsum("tk,lkd->tld", panel_codes.astype(jnp.float32), panel_weight.astype(jnp.float32))
        return carry + term.astype(jnp.bfloat16).astype(jnp.float32), None

    total, _ = lax.scan(decode_panel, jnp.zeros((TOKENS, LAYERS, D), jnp.float32), (code_panels, dec_panels))
    return (total + dec_bias[None, :, :]).astype(jnp.bfloat16)
```

```python
import jax
import jax.numpy as jnp
from jax import lax
from jax.sharding import PartitionSpec as P


def partners(count):
    pairs = count // 2
    if pairs & (pairs - 1):
        return [[(i, (i + 2 * k) % count) for i in range(count)] for k in range(1, pairs)]
    return [[(i, i ^ (2 * k)) for i in range(count)] for k in range(1, pairs)]


def make(mesh):
    latent = mesh.shape["latent"]
    swap = [(i, i ^ 1) for i in range(latent)]
    rounds = partners(latent)
    back = [[(j, i) for i, j in table] for table in rounds]

    def on_device(acts, enc_weight, enc_bias, dec_weight, dec_bias):
        own = acts[:, 0, :]
        rows = own.shape[0]
        shards = [own] + [lax.ppermute(own, "latent", table) for table in rounds]
        near = jnp.concatenate(shards, axis=0)
        far = lax.ppermute(near, "latent", swap)
        tokens = jnp.concatenate([near, far], axis=0)
        pre = jnp.dot(tokens, enc_weight[0], preferred_element_type=jnp.float32)
        shares = lax.all_gather(pre.astype(jnp.bfloat16), "layer", axis=0, tiled=False)
        total = jnp.sum(shares.astype(jnp.float32), axis=0) + enc_bias[None, :]
        codes = jnp.maximum(total, 0.0).astype(jnp.bfloat16)
        half = near.shape[0]
        out = jnp.dot(codes, dec_weight[0], preferred_element_type=jnp.float32).astype(jnp.bfloat16)
        got = lax.ppermute(out[half:], "latent", swap)
        mine = (out[:half].astype(jnp.float32) + got.astype(jnp.float32)).astype(jnp.bfloat16)
        acc = mine[:rows].astype(jnp.float32)
        for k, table in enumerate(back):
            acc = acc + lax.ppermute(mine[(k + 1) * rows : (k + 2) * rows], "latent", table).astype(jnp.float32)
        return (acc + dec_bias).astype(jnp.bfloat16)[:, None, :]

    return on_device


def solution(mesh):
    return jax.shard_map(
        make(mesh),
        mesh=mesh,
        in_specs=(
            P("latent", "layer", None),
            P("layer", None, "latent"),
            P("latent"),
            P("layer", "latent", None),
            P("layer", None),
        ),
        out_specs=P("latent", "layer", None),
        check_vma=False,
    )
```

```python
import jax
import jax.numpy as jnp
from jax import lax
from jax.experimental import pallas as pl
from jax.experimental.pallas import tpu as pltpu
from jax.sharding import PartitionSpec as P


def meetings(count):
    chips = count // 2
    assert chips & (chips - 1) == 0
    return [[(i, i ^ (2 * k + 1)) for i in range(count)] for k in range(chips - 1, 0, -1)]


def doublings(count):
    assert count & (count - 1) == 0
    return [[(i, i ^ (1 << k)) for i in range(count)] for k in range(count.bit_length() - 1)]


def reverse(table):
    return [(j, i) for i, j in table]


def staged(x):
    def body(src, dst, sem):
        copy = pltpu.make_async_copy(src, dst, sem)
        copy.start()
        copy.wait()

    return pl.pallas_call(
        body,
        out_shape=pltpu.VMEM(x.shape, x.dtype),
        in_specs=[pl.BlockSpec(memory_space=pl.ANY)],
        out_specs=pl.BlockSpec(memory_space=pltpu.VMEM),
        scratch_shapes=[pltpu.SemaphoreType.DMA],
        compiler_params=pltpu.CompilerParams(vmem_limit_bytes=4 << 20),
    )(x)


def make(mesh):
    latent, layer = mesh.shape["latent"], mesh.shape["layer"]
    swap = [(i, i ^ 1) for i in range(latent)]
    rounds = meetings(latent)
    steps = doublings(layer)
    cut = len(rounds) // 2

    def on_device(acts, enc_weight, enc_bias, dec_weight, dec_bias):
        own = acts[:, 0, :]
        rows = own.shape[0]

        def encode(shards):
            tokens = jnp.concatenate(shards, axis=0)
            pre = jnp.concatenate(
                [
                    jnp.dot(tokens, enc_near, preferred_element_type=jnp.float32),
                    jnp.dot(tokens, enc_far, preferred_element_type=jnp.float32),
                ],
                axis=0,
            )
            return pre

        def mix(steps, pre):
            for table in steps:
                got = lax.ppermute(pre.astype(jnp.bfloat16), "layer", table)
                pre = pre + got.astype(jnp.float32)
            return pre

        def decode(total):
            half = total.shape[0] // 2
            code = jnp.maximum(total[:half] + enc_bias[None, :], 0.0).astype(jnp.bfloat16)
            code_far = jnp.maximum(total[half:] + bias_far[None, :], 0.0).astype(jnp.bfloat16)
            return jnp.dot(code, dec, preferred_element_type=jnp.float32) + jnp.dot(
                code_far, dec_far, preferred_element_type=jnp.float32
            )

        got = [lax.ppermute(own, "latent", table) for table in rounds]
        enc = enc_weight[0]
        dec = dec_weight[0]
        enc_far = lax.ppermute(enc, "latent", swap)
        dec_far = lax.ppermute(dec, "latent", swap)
        bias_far = lax.ppermute(enc_bias, "latent", swap)
        enc_near = staged(enc)
        first = mix(steps, encode([own] + got[:cut]))
        second = mix(steps[::-1], encode(got[cut:]))
        out = decode(first)
        acc = out[:rows] + dec_bias
        out = out.astype(jnp.bfloat16)
        back = [
            lax.ppermute(out[(k + 1) * rows : (k + 2) * rows], "latent", reverse(table))
            for k, table in enumerate(rounds[:cut])
        ]
        out = decode(second).astype(jnp.bfloat16)
        back += [
            lax.ppermute(out[k * rows : (k + 1) * rows], "latent", reverse(table))
            for k, table in enumerate(rounds[cut:])
        ]
        for part in back:
            acc = acc + part.astype(jnp.float32)
        return acc.astype(jnp.bfloat16)[:, None, :]

    return on_device


def solution(mesh):
    return jax.shard_map(
        make(mesh),
        mesh=mesh,
        in_specs=(
            P("latent", "layer", None),
            P("layer", None, "latent"),
            P("latent"),
            P("layer", "latent", None),
            P("layer", None),
        ),
        out_specs=P("latent", "layer", None),
        check_vma=False,
    )
```

```python
import jax
import jax.numpy as jnp
from jax import lax
from jax.experimental import pallas as pl
from jax.experimental.pallas import tpu as pltpu
from jax.sharding import PartitionSpec as P


def meetings(count):
    chips = count // 2
    assert chips & (chips - 1) == 0
    return [[(i, i ^ (2 * k + 1)) for i in range(count)] for k in range(chips - 1, 0, -1)]


def doublings(count):
    assert count & (count - 1) == 0
    return [[(i, i ^ (1 << k)) for i in range(count)] for k in range(count.bit_length() - 1)]


def reverse(table):
    return [(j, i) for i, j in table]


def staged(x):
    parts = 4 if x.shape[0] % 64 == 0 else 1
    step = x.shape[0] // parts

    def body(src, dst, sems):
        spans = [pl.ds(p * step, step) for p in range(parts)]
        copies = [pltpu.make_async_copy(src.at[s], dst.at[s], sems.at[p]) for p, s in enumerate(spans)]
        for copy in copies:
            copy.start()
        for copy in copies:
            copy.wait()

    return pl.pallas_call(
        body,
        out_shape=pltpu.VMEM(x.shape, x.dtype),
        in_specs=[pl.BlockSpec(memory_space=pltpu.HBM)],
        out_specs=pl.BlockSpec(memory_space=pltpu.VMEM),
        scratch_shapes=[pltpu.SemaphoreType.DMA((parts,))],
        compiler_params=pltpu.CompilerParams(vmem_limit_bytes=56 << 20),
    )(x)


def make(mesh):
    latent, layer = mesh.shape["latent"], mesh.shape["layer"]
    swap = [(i, i ^ 1) for i in range(latent)]
    rounds = meetings(latent)
    steps = doublings(layer)
    cut = len(rounds) // 2

    def on_device(acts, enc_weight, enc_bias, dec_weight, dec_bias):
        own = acts[:, 0, :]
        rows = own.shape[0]

        def encode(shards):
            tokens = jnp.concatenate(shards, axis=0)
            pre = jnp.concatenate(
                [
                    jnp.dot(tokens, enc_near, preferred_element_type=jnp.float32),
                    jnp.dot(tokens, enc_far, preferred_element_type=jnp.float32),
                ],
                axis=0,
            )
            return pre

        def mix(steps, pre):
            for table in steps:
                got = lax.ppermute(pre.astype(jnp.bfloat16), "layer", table)
                pre = pre + got.astype(jnp.float32)
            return pre

        def decode(total):
            half = total.shape[0] // 2
            code = jnp.maximum(total[:half] + enc_bias[None, :], 0.0).astype(jnp.bfloat16)
            code_far = jnp.maximum(total[half:] + bias_far[None, :], 0.0).astype(jnp.bfloat16)
            return jnp.dot(code, dec, preferred_element_type=jnp.float32) + jnp.dot(
                code_far, dec_far, preferred_element_type=jnp.float32
            )

        got = [lax.ppermute(own, "latent", table) for table in rounds]
        enc = enc_weight[0]
        dec = dec_weight[0]
        enc_far = lax.ppermute(enc, "latent", swap)
        dec_far = lax.ppermute(dec, "latent", swap)
        bias_far = lax.ppermute(enc_bias, "latent", swap)
        enc_near = staged(enc)
        first = mix(steps, encode([own] + got[:cut]))
        second = mix(steps[::-1], encode(got[cut:]))
        out = decode(first)
        acc = out[:rows] + dec_bias
        out = out.astype(jnp.bfloat16)
        back = [
            lax.ppermute(out[(k + 1) * rows : (k + 2) * rows], "latent", reverse(table))
            for k, table in enumerate(rounds[:cut])
        ]
        out = decode(second).astype(jnp.bfloat16)
        back += [
            lax.ppermute(out[k * rows : (k + 1) * rows], "latent", reverse(table))
            for k, table in enumerate(rounds[cut:])
        ]
        for part in back:
            acc = acc + part.astype(jnp.float32)
        return acc.astype(jnp.bfloat16)[:, None, :]

    return on_device


def solution(mesh):
    return jax.shard_map(
        make(mesh),
        mesh=mesh,
        in_specs=(
            P("latent", "layer", None),
            P("layer", None, "latent"),
            P("latent"),
            P("layer", "latent", None),
            P("layer", None),
        ),
        out_specs=P("latent", "layer", None),
        check_vma=False,
    )
```

```python
import jax
import jax.numpy as jnp
from jax import lax
from jax.experimental import pallas as pl
from jax.experimental.pallas import tpu as pltpu
from jax.sharding import PartitionSpec as P


def meetings(count):
    chips = count // 2
    assert chips & (chips - 1) == 0
    return [[(i, i ^ (2 * k + 1)) for i in range(count)] for k in range(chips - 1, 0, -1)]


def doublings(count):
    assert count & (count - 1) == 0
    return [[(i, i ^ (1 << k)) for i in range(count)] for k in range(count.bit_length() - 1)]


def reverse(table):
    return [(j, i) for i, j in table]


def staged(x):
    parts = 4 if x.shape[0] % 64 == 0 else 1
    step = x.shape[0] // parts

    def body(src, dst, sems):
        spans = [pl.ds(p * step, step) for p in range(parts)]
        copies = [pltpu.make_async_copy(src.at[s], dst.at[s], sems.at[p]) for p, s in enumerate(spans)]
        for copy in copies:
            copy.start()
        for copy in copies:
            copy.wait()

    return pl.pallas_call(
        body,
        out_shape=pltpu.VMEM(x.shape, x.dtype),
        in_specs=[pl.BlockSpec(memory_space=pltpu.HBM)],
        out_specs=pl.BlockSpec(memory_space=pltpu.VMEM),
        scratch_shapes=[pltpu.SemaphoreType.DMA((parts,))],
        compiler_params=pltpu.CompilerParams(vmem_limit_bytes=56 << 20),
    )(x)


VMEM = pl.BlockSpec(memory_space=pltpu.VMEM)
FLOAT, HALF = jnp.float32, jnp.bfloat16


def product(x, w):
    return jnp.dot(x, w, preferred_element_type=FLOAT)


def encode_call(shards, near, far):
    count, rows, panel = len(shards), sum(x.shape[0] for x in shards), near.shape[1]

    def body(*refs):
        near_ref, far_ref, pre, sent = refs[count:]
        x = jnp.concatenate([ref[...] for ref in refs[:count]], axis=0)
        for p, w in enumerate((near_ref, far_ref)):
            y = product(x, w[...])
            pre[pl.ds(p * rows, rows), :] = y
            sent[pl.ds(p * rows, rows), :] = y.astype(HALF)

    shape = (2 * rows, panel)
    return pl.pallas_call(
        body,
        out_shape=[jax.ShapeDtypeStruct(shape, FLOAT), jax.ShapeDtypeStruct(shape, HALF)],
        in_specs=[VMEM] * (count + 2),
        out_specs=[VMEM] * 2,
        compiler_params=pltpu.CompilerParams(vmem_limit_bytes=16 << 20),
    )(*shards, near, far)


def decode_call(share, other, bias, bias_far, near, far, own, rows):
    half, width = share.shape[0] // 2, near.shape[1]
    kinds = [FLOAT] * own + [HALF] * (half // rows - own)

    def body(share_ref, other_ref, bias_ref, bias_far_ref, near_ref, far_ref, *outs):
        total = share_ref[...] + other_ref[...].astype(FLOAT)
        code = jnp.maximum(total[:half] + bias_ref[...], 0.0).astype(HALF)
        code_far = jnp.maximum(total[half:] + bias_far_ref[...], 0.0).astype(HALF)
        y = product(code, near_ref[...]) + product(code_far, far_ref[...])
        for i, out in enumerate(outs):
            out[...] = y[i * rows : (i + 1) * rows].astype(out.dtype)

    return pl.pallas_call(
        body,
        out_shape=[jax.ShapeDtypeStruct((rows, width), kind) for kind in kinds],
        in_specs=[VMEM] * 6,
        out_specs=[VMEM] * len(kinds),
        compiler_params=pltpu.CompilerParams(vmem_limit_bytes=16 << 20),
    )(share, other, bias[None, :], bias_far[None, :], near, far)


def make(mesh):
    latent, layer = mesh.shape["latent"], mesh.shape["layer"]
    swap = [(i, i ^ 1) for i in range(latent)]
    rounds = meetings(latent)
    steps = doublings(layer)
    cut = len(rounds) // 2

    def on_device(acts, enc_weight, enc_bias, dec_weight, dec_bias):
        own = acts[:, 0, :]
        rows = own.shape[0]

        def permute(x, axis, table):
            return lax.ppermute(x, axis, table)

        def encode(shards):
            return encode_call(shards, enc_near, enc_far)

        def mix(order, pre, sent):
            for k, table in enumerate(order):
                other = permute(sent, "layer", table)
                if k + 1 < len(order):
                    pre = pre + other.astype(FLOAT)
                    sent = pre.astype(HALF)
            return pre, other

        def decode(own_too, share, other):
            return decode_call(share, other, enc_bias, bias_far, dec, dec_far, own_too, rows)

        got = [permute(own, "latent", table) for table in rounds]
        enc = enc_weight[0]
        dec = dec_weight[0]
        enc_far = permute(enc, "latent", swap)
        dec_far = permute(dec, "latent", swap)
        bias_far = permute(enc_bias, "latent", swap)
        enc_near = staged(enc)
        first = mix(steps, *encode([own] + got[:cut]))
        second = mix(steps[::-1], *encode(got[cut:]))
        own_out, *out = decode(1, *first)
        acc = own_out + dec_bias
        back = [permute(out[k], "latent", reverse(table)) for k, table in enumerate(rounds[:cut])]
        out = decode(0, *second)
        back += [permute(out[k], "latent", reverse(table)) for k, table in enumerate(rounds[cut:])]
        for part in back:
            acc = acc + part.astype(jnp.float32)
        return acc.astype(jnp.bfloat16)[:, None, :]

    return on_device


def solution(mesh):
    return jax.shard_map(
        make(mesh),
        mesh=mesh,
        in_specs=(
            P("latent", "layer", None),
            P("layer", None, "latent"),
            P("latent"),
            P("layer", "latent", None),
            P("layer", None),
        ),
        out_specs=P("latent", "layer", None),
        check_vma=False,
    )
```

```python
import jax
import jax.numpy as jnp
from jax import lax
from jax.experimental import pallas as pl
from jax.experimental.pallas import tpu as pltpu
from jax.sharding import PartitionSpec as P


def meetings(count):
    chips = count // 2
    assert chips & (chips - 1) == 0
    return [[(i, i ^ (2 * k + 1)) for i in range(count)] for k in range(chips - 1, 0, -1)]


def doublings(count):
    assert count & (count - 1) == 0
    return [[(i, i ^ (1 << k)) for i in range(count)] for k in range(count.bit_length() - 1)]


def reverse(table):
    return [(j, i) for i, j in table]


def staged(x):
    parts = 4 if x.shape[0] % 64 == 0 else 1
    step = x.shape[0] // parts

    def body(src, dst, sems):
        spans = [pl.ds(p * step, step) for p in range(parts)]
        copies = [pltpu.make_async_copy(src.at[s], dst.at[s], sems.at[p]) for p, s in enumerate(spans)]
        for copy in copies:
            copy.start()
        for copy in copies:
            copy.wait()

    return pl.pallas_call(
        body,
        out_shape=pltpu.VMEM(x.shape, x.dtype),
        in_specs=[pl.BlockSpec(memory_space=pltpu.HBM)],
        out_specs=pl.BlockSpec(memory_space=pltpu.VMEM),
        scratch_shapes=[pltpu.SemaphoreType.DMA((parts,))],
        compiler_params=pltpu.CompilerParams(vmem_limit_bytes=56 << 20),
    )(x)


VMEM = pl.BlockSpec(memory_space=pltpu.VMEM)
FLOAT, HALF = jnp.float32, jnp.bfloat16


def product(x, w):
    return jnp.dot(x, w, preferred_element_type=FLOAT)


def encode_call(shards, near, far):
    count, rows, panel = len(shards), sum(x.shape[0] for x in shards), near.shape[1]

    def body(*refs):
        near_ref, far_ref, pre, sent = refs[count:]
        x = jnp.concatenate([ref[...] for ref in refs[:count]], axis=0)
        for p, w in enumerate((near_ref, far_ref)):
            y = product(x, w[...])
            pre[pl.ds(p * rows, rows), :] = y
            sent[pl.ds(p * rows, rows), :] = y.astype(HALF)

    shape = (2 * rows, panel)
    return pl.pallas_call(
        body,
        out_shape=[jax.ShapeDtypeStruct(shape, FLOAT), jax.ShapeDtypeStruct(shape, HALF)],
        in_specs=[VMEM] * (count + 2),
        out_specs=[VMEM] * 2,
        compiler_params=pltpu.CompilerParams(vmem_limit_bytes=16 << 20),
    )(*shards, near, far)


def decode_call(share, other, bias, bias_far, near, far, own, rows):
    half, width = share.shape[0] // 2, near.shape[1]
    kinds = [FLOAT] * own + [HALF] * (half // rows - own)

    def body(share_ref, other_ref, bias_ref, bias_far_ref, near_ref, far_ref, *outs):
        total = share_ref[...] + other_ref[...].astype(FLOAT)
        code = jnp.maximum(total[:half] + bias_ref[...], 0.0).astype(HALF)
        code_far = jnp.maximum(total[half:] + bias_far_ref[...], 0.0).astype(HALF)
        y = product(code, near_ref[...]) + product(code_far, far_ref[...])
        for i, out in enumerate(outs):
            out[...] = y[i * rows : (i + 1) * rows].astype(out.dtype)

    return pl.pallas_call(
        body,
        out_shape=[jax.ShapeDtypeStruct((rows, width), kind) for kind in kinds],
        in_specs=[VMEM] * 6,
        out_specs=[VMEM] * len(kinds),
        compiler_params=pltpu.CompilerParams(vmem_limit_bytes=16 << 20),
    )(share, other, bias[None, :], bias_far[None, :], near, far)


def finish_call(own, bias, parts):
    rows, width = own.shape
    blocks = 3 if width % 384 == 0 else 1
    block, count = width // blocks, len(parts)

    def body(own_ref, bias_ref, *refs):
        out, held, sems = refs[count:]
        copies = []
        for b in range(blocks):
            span = pl.ds(b * block, block)
            total = own_ref[:, span] + bias_ref[:, span]
            for ref in refs[:count]:
                total = total + ref[:, span].astype(FLOAT)
            held[:, span] = total.astype(HALF)
            copies.append(pltpu.make_async_copy(held.at[:, span], out.at[:, span], sems.at[b]))
            copies[-1].start()
        for copy in copies:
            copy.wait()

    return pl.pallas_call(
        body,
        out_shape=jax.ShapeDtypeStruct((rows, width), HALF),
        in_specs=[VMEM] * (2 + count),
        out_specs=pl.BlockSpec(memory_space=pltpu.HBM),
        scratch_shapes=[pltpu.VMEM((rows, width), HALF), pltpu.SemaphoreType.DMA((blocks,))],
        compiler_params=pltpu.CompilerParams(vmem_limit_bytes=8 << 20),
    )(own, bias, *parts)


def make(mesh):
    latent, layer = mesh.shape["latent"], mesh.shape["layer"]
    swap = [(i, i ^ 1) for i in range(latent)]
    rounds = meetings(latent)
    steps = doublings(layer)
    cut = len(rounds) // 2

    def on_device(acts, enc_weight, enc_bias, dec_weight, dec_bias):
        own = acts[:, 0, :]
        rows = own.shape[0]

        def permute(x, axis, table):
            return lax.ppermute(x, axis, table)

        def encode(shards):
            return encode_call(shards, enc_near, enc_far)

        def mix(order, pre, sent):
            for k, table in enumerate(order):
                other = permute(sent, "layer", table)
                if k + 1 < len(order):
                    pre = pre + other.astype(FLOAT)
                    sent = pre.astype(HALF)
            return pre, other

        def decode(own_too, share, other):
            return decode_call(share, other, enc_bias, bias_far, dec, dec_far, own_too, rows)

        got = [permute(own, "latent", table) for table in rounds]
        enc = enc_weight[0]
        dec = dec_weight[0]
        enc_far = permute(enc, "latent", swap)
        dec_far = permute(dec, "latent", swap)
        bias_far = permute(enc_bias, "latent", swap)
        enc_near = staged(enc)
        first = mix(steps, *encode([own] + got[:cut]))
        second = mix(steps[::-1], *encode(got[cut:]))
        own_out, *out = decode(1, *first)
        back = [permute(out[k], "latent", reverse(table)) for k, table in enumerate(rounds[:cut])]
        out = decode(0, *second)
        back += [permute(out[k], "latent", reverse(table)) for k, table in enumerate(rounds[cut:])]
        return finish_call(own_out, dec_bias, back)[:, None, :]

    return on_device


def solution(mesh):
    return jax.shard_map(
        make(mesh),
        mesh=mesh,
        in_specs=(
            P("latent", "layer", None),
            P("layer", None, "latent"),
            P("latent"),
            P("layer", "latent", None),
            P("layer", None),
        ),
        out_specs=P("latent", "layer", None),
        check_vma=False,
    )
```
